64 devices in a mesh: dp: 4 (over x, y), cp: 16 (over z, core).
Axes of the slice: x: 2, y: 2, z: 8, core: 2. Of those that a mesh axis runs over, the one named last changes fastest.
The devices are a block of a 4x4x8 slice.
Arguments:
- q_tokens: bfloat16 [24576, 12, 128], P(('dp', 'cp')), parts along dimension 0
- k_tokens: bfloat16 [24576, 2, 128], P(('dp', 'cp')), parts along dimension 0
- v_tokens: bfloat16 [24576, 2, 128], P(('dp', 'cp')), parts along dimension 0
Outputs:
- output 1: bfloat16 [24576, 12, 128], P(('dp', 'cp')), parts along dimension 0
- output 2: float32 [24576, 12], P(('dp', 'cp')), parts along dimension 0
There are 4 independent parts. The reference program is written for one: setup_inputs(seed, part) draws one part's arguments, and reference() takes and returns one part's arrays. A program takes and returns all parts, laid end to end along the dimension named above; each array names one.
All inputs are finite; a program needn't handle non-finite values.
Results may differ from the reference program's by a relative error of at most 0.00257823.
Values are sent between devices in bfloat16 or wider.
A program may use at most 768 MiB of HBM per device.

```python
import jax
import jax.numpy as jnp
from jax import lax

CP = 16
TOKENS_DEV = 384
HEADS = 12
KV_HEADS = 2
HEAD = 128

HALF_LEN = TOKENS_DEV // 2
SEQ_LEN = CP * TOKENS_DEV
N_BLOCKS = 2 * CP
GROUP_SIZE = HEADS // KV_HEADS


def setup_inputs(seed: int = 0, part: int = 0) -> dict:
    root_key = jax.random.fold_in(jax.random.key(seed), part)
    key_q, key_k, key_v, key_off = jax.random.split(root_key, 4)
    q_rows = jax.random.normal(key_q, (SEQ_LEN, HEADS, HEAD), jnp.float32)
    k_rows = jax.random.normal(key_k, (SEQ_LEN, KV_HEADS, HEAD), jnp.float32)
    v_offsets = jax.random.normal(key_off, (N_BLOCKS, 1, KV_HEADS, HEAD), jnp.float32)
    v_noise = 0.5 * jax.random.normal(key_v, (N_BLOCKS, HALF_LEN, KV_HEADS, HEAD), jnp.float32)
    v_rows = (v_noise + v_offsets).reshape(SEQ_LEN, KV_HEADS, HEAD)
    return {
        "q_tokens": q_rows.astype(jnp.bfloat16),
        "k_tokens": k_rows.astype(jnp.bfloat16),
        "v_tokens": v_rows.astype(jnp.bfloat16),
    }


def to_natural(rows):
    paired = rows.reshape((CP, 2, HALF_LEN) + rows.shape[1:])
    return jnp.concatenate([paired[:, 0], paired[::-1, 1]], axis=0)


def to_device_order(blocks):
    paired = jnp.stack([blocks[:CP], blocks[CP:][::-1]], axis=1)
    return paired.reshape((SEQ_LEN,) + blocks.shape[2:])


def reference(q_tokens, k_tokens, v_tokens):
    logit_scale = HEAD ** -0.5
    q_blocks = to_natural(q_tokens).reshape(N_BLOCKS, HALF_LEN, KV_HEADS, GROUP_SIZE, HEAD).astype(jnp.float32)
    k_blocks = to_natural(k_tokens).astype(jnp.float32)
    v_blocks = to_natural(v_tokens).astype(jnp.float32)
    offsets = jnp.arange(HALF_LEN)

    def block_scores(q_blk, q_idx, k_idx):
        scores = jnp.einsum("qhgd,khd->hgqk", q_blk, k_blocks[k_idx]) * logit_scale
        visible = (k_idx * HALF_LEN + offsets)[None, :] <= (q_idx * HALF_LEN + offsets)[:, None]
        return jnp.where(visible, scores, -jnp.inf)

    def one_block(block_in):
        q_idx, q_blk = block_in
        init_max = jnp.full((KV_HEADS, GROUP_SIZE, HALF_LEN), -jnp.inf, jnp.float32)
        row_max = lax.fori_loop(
            0, q_idx + 1,
            lambda k_idx, run_max: jnp.maximum(run_max, jnp.max(block_scores(q_blk, q_idx, k_idx), axis=-1)),
            init_max)

        def accumulate(k_idx, sums):
            row_sum, acc = sums
            expd = jnp.exp(block_scores(q_blk, q_idx, k_idx) - row_max[..., None])
            weights = expd.astype(jnp.bfloat16).astype(jnp.float32)
            acc = acc + jnp.einsum("hgqk,khd->qhgd", weights, v_blocks[k_idx])
            return row_sum + jnp.sum(expd, axis=-1), acc

        zero_sum = jnp.zeros((KV_HEADS, GROUP_SIZE, HALF_LEN), jnp.float32)
        zero_acc = jnp.zeros((HALF_LEN, KV_HEADS, GROUP_SIZE, HEAD), jnp.float32)
        row_sum, acc = lax.fori_loop(0, q_idx + 1, accumulate, (zero_sum, zero_acc))
        out_blk = (acc / jnp.transpose(row_sum, (2, 0, 1))[..., None]).astype(jnp.bfloat16)
        lse_blk = jnp.transpose(row_max + jnp.log(row_sum), (2, 0, 1))
        return out_blk.reshape(HALF_LEN, HEADS, HEAD), lse_blk.reshape(HALF_LEN, HEADS)

    out_blocks, lse_blocks = lax.map(one_block, (jnp.arange(N_BLOCKS), q_blocks))
    return to_device_order(out_blocks), to_device_order(lse_blocks)
```

```python
import functools
import math

import jax
import jax.numpy as jnp
from jax import lax
from jax.experimental import pallas as pl
from jax.experimental.pallas import tpu as pltpu
from jax.sharding import PartitionSpec as P

MESH = pl.DeviceIdType.MESH
F32 = jnp.float32
UP, DOWN = 0, 1
LANES = 256


def attention_kernel(n_cp, q_ref, own_ref, o_ref, lse_ref, kv_buf, acc_ref, max_ref, sum_ref,
                     send_sem, recv_sem, pair_send, pair_recv, own_sem):
    n_z = n_cp // 2
    n_round = n_z - 1
    _, kv_heads, _, half_len, head_dim = own_ref.shape
    group = q_ref.shape[0] // kv_heads
    rows = group * half_len
    coef = head_dim ** -0.5 * math.log2(math.e)
    me = lax.axis_index("cp")
    z, core = me // 2, me % 2
    above = lax.rem(z + 1, n_z) * 2 + core
    below = lax.rem(z + n_z - 1, n_z) * 2 + core
    partner = z * 2 + 1 - core

    barrier = pltpu.get_barrier_semaphore()
    for other in (above, below, partner):
        pl.semaphore_signal(barrier, inc=1, device_id={"cp": other}, device_id_type=MESH)
    pl.semaphore_wait(barrier, 3)

    def ring_copy(src, chip, part, way, index):
        return pltpu.make_async_remote_copy(
            src_ref=src, dst_ref=kv_buf.at[part, chip, core],
            send_sem=send_sem.at[way, index], recv_sem=recv_sem.at[way, index],
            device_id={"cp": above if way == UP else below}, device_id_type=MESH)

    def pair_copy(src, chip, part, way, index):
        return pltpu.make_async_remote_copy(
            src_ref=src, dst_ref=kv_buf.at[part, chip, core],
            send_sem=pair_send.at[way, index], recv_sem=pair_recv.at[way, index],
            device_id={"cp": partner}, device_id_type=MESH)

    def pair_wait(chip, part, way, index):
        pltpu.make_async_remote_copy(
            src_ref=kv_buf.at[part, chip, 1 - core], dst_ref=kv_buf.at[part, chip, 1 - core],
            send_sem=pair_send.at[way, index], recv_sem=pair_recv.at[way, index],
            device_id={"cp": partner}, device_id_type=MESH).wait_recv()

    own_copies = [pltpu.make_async_copy(own_ref.at[part], kv_buf.at[part, z, core], own_sem.at[part])
                  for part in range(2)]
    for part in range(2):
        for way in (UP, DOWN):
            ring_copy(own_ref.at[part], z, part, way, part).start()
        pair_copy(own_ref.at[part], z, part, part, n_round).start()
        own_copies[part].start()

    acc_ref[...] = jnp.zeros_like(acc_ref)
    max_ref[...] = jnp.full_like(max_ref, -jnp.inf)
    sum_ref[...] = jnp.zeros_like(sum_ref)

    tiles = [(head, start, min(LANES, rows - start))
             for head in range(kv_heads) for start in range(0, rows, LANES)]

    def job(chip, part, half, key_pos=None, query_base=None):
        def keys(head, which):
            return kv_buf[part, chip, :, head, which].reshape(2 * half_len, head_dim)

        def scores(tile):
            head, start, size = tile
            q_all = q_ref[head * group:(head + 1) * group, half].reshape(rows, head_dim)
            s = lax.dot_general(keys(head, 0), q_all[start:start + size], (((1,), (1,)), ((), ())),
                                preferred_element_type=F32)
            if key_pos is not None:
                lane = lax.broadcasted_iota(jnp.int32, (1, size), 1) + start
                q_pos = query_base + lane % half_len
                s = jnp.where(key_pos <= q_pos, s, -jnp.inf)
            return s

        ahead = scores(tiles[0])
        for n, (head, start, size) in enumerate(tiles):
            s = ahead
            if n + 1 < len(tiles):
                ahead = scores(tiles[n + 1])
            cols = slice(start, start + size)
            v_t = keys(head, 1).T
            old = max_ref[half, head, :, cols]
            new = jnp.maximum(old, jnp.max(s, axis=0, keepdims=True))
            p = jnp.exp2((s - new) * coef)
            alpha = jnp.exp2((old - new) * coef)
            max_ref[half, head, :, cols] = new
            part_sum = jnp.sum(p.reshape(-1, 8, size), axis=0)
            sum_ref[half, head, :, cols] = sum_ref[half, head, :, cols] * alpha + part_sum
            acc_ref[half, head, :, cols] = acc_ref[half, head, :, cols] * alpha + jnp.dot(
                v_t, p.astype(jnp.bfloat16), preferred_element_type=F32)

    for part in range(2):
        own_copies[part].wait()
        pair_wait(z, part, part, n_round)

    job(z, 0, 1)
    row_id = lax.broadcasted_iota(jnp.int32, (2 * half_len, 1), 0)

    def own_job(part, carry):
        first_block = jnp.where(part == 0, 2 * z, 2 * n_cp - 1 - 2 * z)
        shift = jnp.where(part == 0, 0, 2 * half_len)
        key_pos = first_block * half_len + row_id - jnp.where(row_id >= half_len, shift, 0)
        query_block = jnp.where(part == 0, me, 2 * n_cp - 1 - me)
        job(z, part, part, key_pos, query_block * half_len)
        return carry

    lax.fori_loop(0, 2, own_job, 0)

    def source(rnd, way):
        step = rnd // 2 + 1
        chip = lax.rem(z + n_z - step, n_z) if way == UP else lax.rem(z + step, n_z)
        part = jnp.where(rnd == n_round - 1, way, rnd % 2)
        return chip, part

    def remote_round(rnd, carry):
        for way in (UP, DOWN):
            chip, part = source(rnd, way)
            block = kv_buf.at[part, chip, core]
            ring_copy(block, chip, part, way, rnd).wait_recv()
            pair_copy(block, chip, part, way, rnd).start()
            last_forward = n_round - 3 if way == UP else n_round - 2

            @pl.when((rnd < n_round - 3) | (rnd == last_forward))
            def _():
                ring_copy(block, chip, part, way, jnp.minimum(rnd + 2, n_round - 1)).start()
        for way in (UP, DOWN):
            chip, part = source(rnd, way)
            pair_wait(chip, part, way, rnd)

        def one_job(way, inner):
            step = rnd // 2 + 1
            chip = lax.rem(z + n_z + jnp.where(way == UP, -step, step), n_z)
            kind = jnp.where(rnd == n_round - 1, way, rnd % 2)
            lower = jnp.where(chip < z, 1, 0)
            job(chip, kind * (1 - lower), 1 - kind * lower)
            return inner

        lax.fori_loop(0, 2, one_job, 0)
        return carry

    lax.fori_loop(0, n_round, remote_round, 0)

    for half in range(2):
        for head in range(kv_heads):
            total = jnp.sum(sum_ref[half, head], axis=0, keepdims=True)
            lse = max_ref[half, head] * head_dim ** -0.5 + jnp.log(total)
            inverse = 1.0 / total
            for g in range(group):
                lse_ref[head * group + g, half] = lse[0, g * half_len:(g + 1) * half_len]
            out = (acc_ref[half, head] * inverse).T.astype(jnp.bfloat16)
            o_ref[head * group:(head + 1) * group, half] = out.reshape(group, half_len, head_dim)

    for rnd in range(n_round):
        for way in (UP, DOWN):
            chip, part = source(rnd, way)
            block = kv_buf.at[part, chip, core]
            ring_copy(block, chip, part, way, rnd).wait_send()
            pair_copy(block, chip, part, way, rnd).wait_send()
    for part in range(2):
        pair_copy(own_ref.at[part], z, part, part, n_round).wait_send()


def solution(mesh):
    n_cp = mesh.shape["cp"]
    row_spec = P(("dp", "cp"), None, None)
    lse_spec = P(("dp", "cp"), None)

    def local_attention(q_tok, k_tok, v_tok):
        tok_count, q_heads, head_dim = q_tok.shape
        kv_heads = k_tok.shape[1]
        group = q_heads // kv_heads
        half_len = tok_count // 2
        rows = group * half_len
        q_in = q_tok.transpose(1, 0, 2).reshape(q_heads, 2, half_len, head_dim)
        kv = jnp.stack([k_tok, v_tok]).reshape(2, 2, half_len, kv_heads, head_dim)
        own = kv.transpose(1, 3, 0, 2, 4)
        vmem = pl.BlockSpec(memory_space=pltpu.VMEM)
        out, lse = pl.pallas_call(
            functools.partial(attention_kernel, n_cp),
            out_shape=(jax.ShapeDtypeStruct((q_heads, 2, half_len, head_dim), jnp.bfloat16),
                       jax.ShapeDtypeStruct((q_heads, 2, half_len), F32)),
            in_specs=[vmem, vmem],
            out_specs=(vmem, vmem),
            scratch_shapes=[
                pltpu.VMEM((2, n_cp // 2, 2, kv_heads, 2, half_len, head_dim), jnp.bfloat16),
                pltpu.VMEM((2, kv_heads, head_dim, rows), F32),
                pltpu.VMEM((2, kv_heads, 1, rows), F32),
                pltpu.VMEM((2, kv_heads, 8, rows), F32),
                pltpu.SemaphoreType.DMA((2, n_cp // 2 - 1)),
                pltpu.SemaphoreType.DMA((2, n_cp // 2 - 1)),
                pltpu.SemaphoreType.DMA((2, n_cp // 2)),
                pltpu.SemaphoreType.DMA((2, n_cp // 2)),
                pltpu.SemaphoreType.DMA((2,)),
            ],
            compiler_params=pltpu.CompilerParams(collective_id=0, has_side_effects=True,
                                                 vmem_limit_bytes=48 * 1024 * 1024),
        )(q_in, own)
        out_tok = out.reshape(q_heads, tok_count, head_dim).transpose(1, 0, 2)
        return out_tok, lse.reshape(q_heads, tok_count).T

    return jax.shard_map(local_attention, mesh=mesh, in_specs=(row_spec, row_spec, row_spec),
                         out_specs=(row_spec, lse_spec), check_vma=False)
```

```python
import functools
import math

import jax
import jax.numpy as jnp
from jax import lax
from jax.experimental import pallas as pl
from jax.experimental.pallas import tpu as pltpu
from jax.sharding import PartitionSpec as P

MESH = pl.DeviceIdType.MESH
F32 = jnp.float32
BF16 = jnp.bfloat16
UP, DOWN = 0, 1
LANES = 256
DEPTH = 3


def attention_kernel(n_cp, q_hbm, k_hbm, v_hbm, o_ref, lse_ref, q_ref, kv_buf, raw_ref, wide_ref, acc_ref, max_ref,
                     sum_ref, send_sem, recv_sem, pair_send, pair_recv, own_sem):
    n_z = n_cp // 2
    n_round = n_z - 1
    kv_heads, _, half_len, head_dim = kv_buf.shape[3:]
    n_item = n_round * kv_heads
    group = q_ref.shape[0] // kv_heads
    rows = group * half_len
    scale = head_dim ** -0.5
    coef = scale * math.log2(math.e)
    me = lax.axis_index("cp")
    z, core = me // 2, me % 2
    above = lax.rem(z + 1, n_z) * 2 + core
    below = lax.rem(z + n_z - 1, n_z) * 2 + core
    partner = z * 2 + 1 - core

    raw_copies = [pltpu.make_async_copy(src, raw_ref.at[which], own_sem.at[which])
                  for which, src in enumerate((k_hbm, v_hbm))]
    for copy in raw_copies:
        copy.start()
    barrier = pltpu.get_barrier_semaphore()
    for other in (above, below, partner):
        pl.semaphore_signal(barrier, inc=1, device_id={"cp": other}, device_id_type=MESH)
    q_copy = pltpu.make_async_copy(q_hbm, q_ref, own_sem.at[2])
    q_copy.start()

    def ring_copy(chip, part, head, way, index):
        block = kv_buf.at[part, chip, core, head]
        return pltpu.make_async_remote_copy(
            src_ref=block, dst_ref=block, send_sem=send_sem.at[way, index], recv_sem=recv_sem.at[way, index],
            device_id={"cp": jnp.where(way == UP, above, below)}, device_id_type=MESH)

    def pair_copy(chip, part, head, way, index, side):
        block = kv_buf.at[part, chip, side, head]
        return pltpu.make_async_remote_copy(
            src_ref=block, dst_ref=block, send_sem=pair_send.at[way, index], recv_sem=pair_recv.at[way, index],
            device_id={"cp": partner}, device_id_type=MESH)

    for copy in raw_copies:
        copy.wait()

    def split_heads(part):
        span = pl.ds(part * kv_heads * half_len, kv_heads * half_len)
        wide_ref[:, span] = raw_ref[:, span].astype(F32)
        for head in range(kv_heads):
            for which in range(2):
                start = part * kv_heads * half_len + head
                picked = wide_ref[which, pl.ds(start, half_len, stride=kv_heads), :]
                kv_buf[part, z, core, head, which] = picked.astype(BF16)

    for part in range(2):
        split_heads(part)
        if part == 0:
            pl.semaphore_wait(barrier, 3)
        for head in range(kv_heads):
            for way in (UP, DOWN):
                ring_copy(z, part, head, way, part * kv_heads + head).start()
            pair_copy(z, part, head, part, n_item + head, core).start()

    acc_ref[...] = jnp.zeros_like(acc_ref)
    max_ref[...] = jnp.full_like(max_ref, -jnp.inf)
    sum_ref[...] = jnp.zeros_like(sum_ref)

    cuts = [(start, min(LANES, rows - start)) for start in range(0, rows, LANES)]

    def run_jobs(jobs, mask=None):
        tiles = [(job, start, size) for job in jobs for start, size in cuts]

        def keys(job, which):
            chip, part, _, head = job
            return kv_buf[part, chip, :, head, which].reshape(2 * half_len, head_dim)

        def scores(tile):
            job, start, size = tile
            _, _, half, head = job
            q_all = q_ref[pl.ds(head * group, group), half].reshape(rows, head_dim)
            s = lax.dot_general(keys(job, 0), q_all[start:start + size], (((1,), (1,)), ((), ())),
                                preferred_element_type=F32)
            if mask is not None:
                key_pos, query_base = mask
                lane = lax.broadcasted_iota(jnp.int32, (1, size), 1) + start
                s = jnp.where(key_pos <= query_base + lane % half_len, s, -jnp.inf)
            return s

        ahead = [scores(tile) for tile in tiles[:DEPTH]]
        for n, (job, start, size) in enumerate(tiles):
            _, _, half, head = job
            s = ahead.pop(0)
            if n + DEPTH < len(tiles):
                ahead.append(scores(tiles[n + DEPTH]))
            cols = slice(start, start + size)
            v_t = keys(job, 1).T
            old = max_ref[half, head, :, cols]
            new = jnp.maximum(old, jnp.max(s, axis=0, keepdims=True))
            p = jnp.exp2((s - new) * coef)
            alpha = jnp.exp2((old - new) * coef)
            max_ref[half, head, :, cols] = new
            part_sum = jnp.sum(p.reshape(-1, 8, size), axis=0)
            sum_ref[half, head, :, cols] = sum_ref[half, head, :, cols] * alpha + part_sum
            acc_ref[half, head, :, cols] = acc_ref[half, head, :, cols] * alpha + jnp.dot(
                v_t, p.astype(BF16), preferred_element_type=F32)

    def finish(half):
        for head in range(kv_heads):
            total = jnp.sum(sum_ref[half, head], axis=0, keepdims=True)
            lse = max_ref[half, head] * scale + jnp.log(total)
            inverse = 1.0 / total
            for g in range(group):
                lse_ref[head * group + g, half * half_len:(half + 1) * half_len] = (
                    lse[0, g * half_len:(g + 1) * half_len])
            out = (acc_ref[half, head] * inverse).astype(BF16).T
            o_ref[head * group:(head + 1) * group, half] = out.reshape(group, half_len, head_dim)

    q_copy.wait()
    for part in range(2):
        for head in range(kv_heads):
            pair_copy(z, part, head, part, n_item + head, 1 - core).wait_recv()

    def own_open(head, carry):
        run_jobs([(z, 0, 1, head)])
        return carry

    lax.fori_loop(0, kv_heads, own_open, 0)
    row_id = lax.broadcasted_iota(jnp.int32, (2 * half_len, 1), 0)

    def own_masked(item, carry):
        part, head = item // kv_heads, item % kv_heads
        first_block = jnp.where(part == 0, 2 * z, 2 * n_cp - 1 - 2 * z)
        shift = jnp.where(part == 0, 0, 2 * half_len)
        key_pos = first_block * half_len + row_id - jnp.where(row_id >= half_len, shift, 0)
        query_block = jnp.where(part == 0, me, 2 * n_cp - 1 - me)
        run_jobs([(z, part, part, head)], (key_pos, query_block * half_len))
        return carry

    lax.fori_loop(0, 2 * kv_heads, own_masked, 0)

    def place(item, way):
        rnd, head = item // kv_heads, item % kv_heads
        chip = lax.rem(z + n_z + (2 * way - 1) * (rnd // 2 + 1), n_z)
        part = jnp.where(rnd == n_round - 1, way, rnd % 2)
        return rnd, head, chip, part

    def arrive(item, way):
        rnd, head, chip, part = place(item, way)
        ring_copy(chip, part, head, way, item).wait_recv()
        onward = jnp.minimum(rnd + 2, n_round - 1) * kv_heads + head

        @pl.when((rnd < n_round - 3) | (rnd == n_round - 3 + way))
        def _():
            ring_copy(chip, part, head, way, onward).start()

        pair_copy(chip, part, head, way, item, core).start()

    def remote_step(item, carry):
        @pl.when(item < n_item)
        def _():
            for way in (UP, DOWN):
                arrive(item, way)

        @pl.when(item > 0)
        def _():
            jobs = []
            for way in (UP, DOWN):
                _, head, chip, part = place(item - 1, way)
                pair_copy(chip, part, head, way, item - 1, 1 - core).wait_recv()
                lower = jnp.where(chip < z, 1, 0)
                jobs.append((chip, part * (1 - lower), 1 - part * lower, head))
            run_jobs(jobs)

        @pl.when(item == jnp.minimum(2 * kv_heads * z, n_item))
        def _():
            finish(0)
        return carry

    lax.fori_loop(0, n_item + 1, remote_step, 0)
    finish(1)

    for way in (UP, DOWN):
        for item in range(n_item):
            ring_copy(z, 0, 0, way, item).wait_send()
            pair_copy(z, 0, 0, way, item, core).wait_send()
        for head in range(kv_heads):
            pair_copy(z, 0, 0, way, n_item + head, core).wait_send()


def store_kernel(o_ref, lse_ref, o_hbm, lse_hbm, sems):
    copies = [pltpu.make_async_copy(o_ref, o_hbm, sems.at[0]), pltpu.make_async_copy(lse_ref, lse_hbm, sems.at[1])]
    for copy in copies:
        copy.start()
    for copy in copies:
        copy.wait()


def solution(mesh):
    n_cp = mesh.shape["cp"]
    row_spec = P(("dp", "cp"), None, None)
    lse_spec = P(("dp", "cp"), None)

    def local_attention(q_tok, k_tok, v_tok):
        tok_count, q_heads, head_dim = q_tok.shape
        kv_heads = k_tok.shape[1]
        group = q_heads // kv_heads
        half_len = tok_count // 2
        rows = group * half_len
        n_item = (n_cp // 2 - 1) * kv_heads
        q_in = q_tok.transpose(1, 0, 2).reshape(q_heads, 2, half_len, head_dim)
        k_in = k_tok.reshape(tok_count * kv_heads, head_dim)
        v_in = v_tok.reshape(tok_count * kv_heads, head_dim)
        q_in, k_in, v_in = (pltpu.with_memory_space_constraint(x, pltpu.HBM) for x in (q_in, k_in, v_in))
        vmem = pl.BlockSpec(memory_space=pltpu.VMEM)
        hbm = pl.BlockSpec(memory_space=pltpu.HBM)
        out, lse = pl.pallas_call(
            functools.partial(attention_kernel, n_cp),
            out_shape=(pltpu.VMEM(q_in.shape, BF16), pltpu.VMEM((q_heads, tok_count), F32)),
            in_specs=[hbm, hbm, hbm],
            out_specs=(vmem, vmem),
            scratch_shapes=[
                pltpu.VMEM(q_in.shape, BF16),
                pltpu.VMEM((2, n_cp // 2, 2, kv_heads, 2, half_len, head_dim), BF16),
                pltpu.VMEM((2, tok_count * kv_heads, head_dim), BF16),
                pltpu.VMEM((2, tok_count * kv_heads, head_dim), F32),
                pltpu.VMEM((2, kv_heads, head_dim, rows), F32),
                pltpu.VMEM((2, kv_heads, 1, rows), F32),
                pltpu.VMEM((2, kv_heads, 8, rows), F32),
                pltpu.SemaphoreType.DMA((2, n_item)),
                pltpu.SemaphoreType.DMA((2, n_item)),
                pltpu.SemaphoreType.DMA((2, n_item + kv_heads)),
                pltpu.SemaphoreType.DMA((2, n_item + kv_heads)),
                pltpu.SemaphoreType.DMA((3,)),
            ],
            compiler_params=pltpu.CompilerParams(
                collective_id=0, has_side_effects=True,
                vmem_limit_bytes=48 * 1024 * 1024),
        )(q_in, k_in, v_in)
        out, lse = pl.pallas_call(
            store_kernel,
            out_shape=(jax.ShapeDtypeStruct(out.shape, BF16), jax.ShapeDtypeStruct(lse.shape, F32)),
            in_specs=[vmem, vmem],
            out_specs=(hbm, hbm),
            scratch_shapes=[pltpu.SemaphoreType.DMA((2,))],
            compiler_params=pltpu.CompilerParams(vmem_limit_bytes=48 * 1024 * 1024),
        )(out, lse)
        out_tok = out.reshape(q_heads, tok_count, head_dim).transpose(1, 0, 2)
        return out_tok, lse.T

    return jax.shard_map(local_attention, mesh=mesh, in_specs=(row_spec, row_spec, row_spec),
                         out_specs=(row_spec, lse_spec), check_vma=False)
```

```python
import functools
import math

import jax
import jax.numpy as jnp
from jax import lax
from jax.experimental import pallas as pl
from jax.experimental.pallas import tpu as pltpu
from jax.sharding import PartitionSpec as P

MESH = pl.DeviceIdType.MESH
F32 = jnp.float32
BF16 = jnp.bfloat16
UP, DOWN = 0, 1
LANES = 256
DEPTH = 3
FAR_UP = 0
SWAP = 0
LAG_UP, LAG_DOWN = -1, 3


def attention_kernel(n_cp, q_hbm, k_hbm, v_hbm, o_ref, lse_ref, q_ref, kv_buf, raw_ref, wide_ref, acc_ref, max_ref,
                     sum_ref, send_sem, recv_sem, pair_send, pair_recv, own_sem):
    n_z = n_cp // 2
    kv_heads, _, _, half_len, head_dim = kv_buf.shape[2:]
    n_base = (n_z - 2) * kv_heads
    n_item = n_base + 2 * kv_heads
    group = q_ref.shape[0] // kv_heads
    rows = group * half_len
    scale = head_dim ** -0.5
    coef = scale * math.log2(math.e)
    me = lax.axis_index("cp")
    z, core = me // 2, me % 2
    way = core if SWAP == 0 else 1 - core
    above = lax.rem(z + 1, n_z) * 2 + core
    below = lax.rem(z + n_z - 1, n_z) * 2 + core
    ahead_id = jnp.where(way == UP, above, below)
    behind_id = jnp.where(way == UP, below, above)
    partner = z * 2 + 1 - core
    z_next = ahead_id // 2

    raw_copies = [pltpu.make_async_copy(src, raw_ref.at[which], own_sem.at[which])
                  for which, src in enumerate((k_hbm, v_hbm))]
    for copy in raw_copies:
        copy.start()
    barrier = pltpu.get_barrier_semaphore()
    for other in (behind_id, partner):
        pl.semaphore_signal(barrier, inc=1, device_id={"cp": other}, device_id_type=MESH)
    q_copy = pltpu.make_async_copy(q_hbm, q_ref, own_sem.at[2])
    q_copy.start()

    def far_early(ring):
        return jnp.where(ring == UP, FAR_UP, kv_heads - FAR_UP)

    def place(item, ring):
        rnd = item // kv_heads
        extra = item - n_base
        early = far_early(ring)
        chip = lax.rem(z + n_z + (2 * ring - 1) * (rnd // 2 + 1), n_z)
        far_chip = lax.rem(z + n_z // 2, n_z)
        far_part = jnp.where(extra < early, 0, 1)
        far_head = jnp.where(extra < early, extra + jnp.where(ring == UP, kv_heads - FAR_UP, 0), extra - early)
        far = item >= n_base
        return (jnp.where(far, far_part, rnd % 2), jnp.where(far, far_chip, chip),
                jnp.where(far, far_head, item % kv_heads))

    def far_ring(chip_to):
        return jnp.where((chip_to > 1) & (chip_to < n_z // 2), UP, DOWN)

    def travels(item, ring, chip_to):
        step = item // kv_heads // 2 + 1
        extra = item - n_base
        early = far_early(ring)
        source = lax.rem(chip_to + n_z - step, n_z)
        near = jnp.where(ring == UP, source > n_z // 2, chip_to + step < n_z)
        far = (ring == far_ring(chip_to)) & (chip_to < n_z // 2) & (extra < early + kv_heads)
        return jnp.where(extra < 0, ((item // kv_heads) % 2 == 0) | near, (extra < early) | far)

    def useful(item, ring):
        part, chip, _ = place(item, ring)
        return travels(item, ring, z) & ((part == 0) | (chip > z))

    def ring_copy(block, item):
        return pltpu.make_async_remote_copy(
            src_ref=block, dst_ref=block, send_sem=send_sem.at[item], recv_sem=recv_sem.at[item],
            device_id={"cp": ahead_id}, device_id_type=MESH)

    def pair_copy(block, item):
        return pltpu.make_async_remote_copy(
            src_ref=block, dst_ref=block, send_sem=pair_send.at[item], recv_sem=pair_recv.at[item],
            device_id={"cp": partner}, device_id_type=MESH)

    for copy in raw_copies:
        copy.wait()

    def split_heads(part):
        span = pl.ds(part * kv_heads * half_len, kv_heads * half_len)
        wide_ref[:, span] = raw_ref[:, span].astype(F32)
        for head in range(kv_heads):
            for which in range(2):
                start = part * kv_heads * half_len + head
                picked = wide_ref[which, pl.ds(start, half_len, stride=kv_heads), :]
                kv_buf[part, z, head, core, which] = picked.astype(BF16)

    def send_own(part, side):
        @pl.when(travels(part * kv_heads, way, z_next))
        def _():
            for head in range(kv_heads):
                ring_copy(kv_buf.at[part, z, head, side], part * kv_heads + head).start()

    for part in range(2):
        split_heads(part)
        if part == 0:
            pl.semaphore_wait(barrier, 2)
        for head in range(kv_heads):
            pair_copy(kv_buf.at[part, z, head, core], n_item + part * kv_heads + head).start()
        if part == 0:
            send_own(part, core)

    for part in range(2):
        if part > 0:
            send_own(part, core)
        for head in range(kv_heads):
            pair_copy(kv_buf.at[part, z, head, 1 - core], n_item + part * kv_heads + head).wait_recv()
        send_own(part, 1 - core)

    acc_ref[...] = jnp.zeros_like(acc_ref)
    max_ref[...] = jnp.full_like(max_ref, -jnp.inf)
    sum_ref[...] = jnp.zeros_like(sum_ref)

    cuts = [(start, min(LANES, rows - start)) for start in range(0, rows, LANES)]

    def run_jobs(jobs, mask=None):
        tiles = [(job, start, size) for start, size in cuts for job in jobs]

        def keys(job, which):
            chip, part, _, head = job
            return kv_buf[part, chip, head, :, which].reshape(2 * half_len, head_dim)

        def scores(tile):
            job, start, size = tile
            _, _, half, head = job
            q_all = q_ref[pl.ds(head * group, group), half].reshape(rows, head_dim)
            s = lax.dot_general(keys(job, 0), q_all[start:start + size], (((1,), (1,)), ((), ())),
                                preferred_element_type=F32)
            if mask is not None:
                key_pos, query_base = mask
                lane = lax.broadcasted_iota(jnp.int32, (1, size), 1) + start
                s = jnp.where(key_pos <= query_base + lane % half_len, s, -jnp.inf)
            return s

        ahead = [scores(tile) for tile in tiles[:DEPTH]]
        for n, (job, start, size) in enumerate(tiles):
            _, _, half, head = job
            s = ahead.pop(0)
            if n + DEPTH < len(tiles):
                ahead.append(scores(tiles[n + DEPTH]))
            cols = slice(start, start + size)
            v_t = keys(job, 1).T
            old = max_ref[half, head, :, cols]
            new = jnp.maximum(old, jnp.max(s, axis=0, keepdims=True))
            p = jnp.exp2((s - new) * coef)
            alpha = jnp.exp2((old - new) * coef)
            max_ref[half, head, :, cols] = new
            part_sum = jnp.sum(p.reshape(-1, 8, size), axis=0)
            sum_ref[half, head, :, cols] = sum_ref[half, head, :, cols] * alpha + part_sum
            acc_ref[half, head, :, cols] = acc_ref[half, head, :, cols] * alpha + jnp.dot(
                v_t, p.astype(BF16), preferred_element_type=F32)

    def finish(half, heads):
        for head in heads:
            total = jnp.sum(sum_ref[half, head], axis=0, keepdims=True)
            lse = max_ref[half, head] * scale + jnp.log(total)
            inverse = 1.0 / total
            for g in range(group):
                lse_ref[head * group + g, half * half_len:(half + 1) * half_len] = (
                    lse[0, g * half_len:(g + 1) * half_len])
            out = (acc_ref[half, head] * inverse).astype(BF16).T
            o_ref[head * group:(head + 1) * group, half] = out.reshape(group, half_len, head_dim)

    q_copy.wait()

    row_id = lax.broadcasted_iota(jnp.int32, (2 * half_len, 1), 0)

    def own_masked(item, carry):
        part, head = item // kv_heads, item % kv_heads
        first_block = jnp.where(part == 0, 2 * z, 2 * n_cp - 1 - 2 * z)
        shift = jnp.where(part == 0, 0, 2 * half_len)
        key_pos = first_block * half_len + row_id - jnp.where(row_id >= half_len, shift, 0)
        query_block = jnp.where(part == 0, me, 2 * n_cp - 1 - me)
        run_jobs([(z, part, part, head)], (key_pos, query_block * half_len))
        return carry

    lax.fori_loop(0, 2 * kv_heads, own_masked, 0)

    def arrive(item):
        part, chip, head = place(item, way)
        block = kv_buf.at[part, chip, head]
        ring_copy(block, item).wait_recv()
        final = item - (n_base - 2 * kv_heads)
        first_far = jnp.where(way == UP, kv_heads - FAR_UP, 0)
        stays = (final >= 0) & (part == 0) & ((head < first_far) | (head >= first_far + far_early(way)))
        onward = jnp.where(final < 0, item + 2 * kv_heads,
                           n_base + head + jnp.where(part == 0, -first_far, far_early(way)))

        @pl.when((item < n_base) & jnp.logical_not(stays) & travels(onward, way, z_next))
        def _():
            ring_copy(block, onward).start()

        @pl.when(useful(item, way))
        def _():
            pair_copy(block, item).start()

    def job_of(item, ring):
        part, chip, head = place(jnp.maximum(item, 0), ring)
        lower = jnp.where(chip < z, 1, 0)
        remote = (chip, part * (1 - lower), 1 - part * lower, head)
        opening = (z, 0, 1, -1 - item)
        return tuple(jnp.where(item >= 0, b, a) for a, b in zip(opening, remote))

    def count(ring):
        return n_base + far_early(ring) + jnp.where(ring == far_ring(z), kv_heads, 0)

    early_up = (z == 0) & (way == UP)
    lag = jnp.where(z == 0, jnp.where(way == UP, LAG_UP, LAG_DOWN), 1)

    def remote_step(turn, carry):
        tick = turn - 4

        def fetch(item, ring, mine):
            @pl.when(mine & travels(item, ring, z))
            def _():
                arrive(item)

            @pl.when(jnp.logical_not(mine) & (item >= 0) & useful(item, ring))
            def _():
                pair_copy(kv_buf.at[place(item, ring)], item).wait_recv()

        def valid(item, ring, first):
            return (item >= first) & (item < count(ring))

        both = valid(tick, way, 0) & valid(tick - lag, 1 - way, -kv_heads) & jnp.logical_not(early_up & (tick >= n_base))

        @pl.when(both)
        def _():
            @pl.when(travels(tick, way, z))
            def _():
                arrive(tick)

            @pl.when((tick >= lag) & useful(tick - lag, 1 - way))
            def _():
                pair_copy(kv_buf.at[place(tick - lag, 1 - way)], tick - lag).wait_recv()

            run_jobs([job_of(tick, way), job_of(tick - lag, 1 - way)])

        def slot(which, inner):
            mine = which == jnp.where(early_up, 1, 0)
            item = jnp.where(mine, tick, tick - lag)
            ring = jnp.where(mine, way, 1 - way)

            @pl.when(valid(item, ring, jnp.where(mine, 0, -kv_heads)))
            def _():
                fetch(item, ring, mine)
                run_jobs([job_of(item, ring)])
            return inner

        @pl.when(jnp.logical_not(both))
        def _():
            lax.fori_loop(0, 2, slot, 0)

        @pl.when(tick == 2 * kv_heads * z)
        def _():
            finish(0, range(kv_heads))
        return carry

    lax.fori_loop(0, n_item + 7, remote_step, 0)

    @pl.when(z >= n_z // 2)
    def _():
        finish(0, range(kv_heads))

    finish(1, range(kv_heads))

    def drain(item, carry):
        block = kv_buf.at[0, z, 0]

        @pl.when(travels(item, way, z_next))
        def _():
            ring_copy(block, item).wait_send()

        @pl.when(useful(item, way))
        def _():
            pair_copy(block, item).wait_send()
        return carry

    lax.fori_loop(0, n_item, drain, 0)
    for item in range(2 * kv_heads):
        pair_copy(kv_buf.at[0, z, 0, core], n_item + item).wait_send()


def store_kernel(o_ref, lse_ref, o_hbm, lse_hbm, sems):
    copies = [pltpu.make_async_copy(o_ref.at[head], o_hbm.at[head], sems.at[head]) for head in range(o_ref.shape[0])]
    copies.append(pltpu.make_async_copy(lse_ref, lse_hbm, sems.at[o_ref.shape[0]]))
    for copy in copies:
        copy.start()
    for copy in copies:
        copy.wait()


def solution(mesh):
    n_cp = mesh.shape["cp"]
    row_spec = P(("dp", "cp"), None, None)
    lse_spec = P(("dp", "cp"), None)

    def local_attention(q_tok, k_tok, v_tok):
        tok_count, q_heads, head_dim = q_tok.shape
        kv_heads = k_tok.shape[1]
        group = q_heads // kv_heads
        half_len = tok_count // 2
        rows = group * half_len
        n_item = n_cp // 2 * kv_heads
        q_in = q_tok.transpose(1, 0, 2).reshape(q_heads, 2, half_len, head_dim)
        k_in = k_tok.reshape(tok_count * kv_heads, head_dim)
        v_in = v_tok.reshape(tok_count * kv_heads, head_dim)
        q_in, k_in, v_in = (pltpu.with_memory_space_constraint(x, pltpu.HBM) for x in (q_in, k_in, v_in))
        vmem = pl.BlockSpec(memory_space=pltpu.VMEM)
        hbm = pl.BlockSpec(memory_space=pltpu.HBM)
        out, lse = pl.pallas_call(
            functools.partial(attention_kernel, n_cp),
            out_shape=(pltpu.VMEM(q_in.shape, BF16), pltpu.VMEM((q_heads, tok_count), F32)),
            in_specs=[hbm, hbm, hbm],
            out_specs=(vmem, vmem),
            scratch_shapes=[
                pltpu.VMEM(q_in.shape, BF16),
                pltpu.VMEM((2, n_cp // 2, kv_heads, 2, 2, half_len, head_dim), BF16),
                pltpu.VMEM((2, tok_count * kv_heads, head_dim), BF16),
                pltpu.VMEM((2, tok_count * kv_heads, head_dim), F32),
                pltpu.VMEM((2, kv_heads, head_dim, rows), F32),
                pltpu.VMEM((2, kv_heads, 1, rows), F32),
                pltpu.VMEM((2, kv_heads, 8, rows), F32),
                pltpu.SemaphoreType.DMA((n_item,)),
                pltpu.SemaphoreType.DMA((n_item,)),
                pltpu.SemaphoreType.DMA((n_item + 2 * kv_heads,)),
                pltpu.SemaphoreType.DMA((n_item + 2 * kv_heads,)),
                pltpu.SemaphoreType.DMA((3,)),
            ],
            compiler_params=pltpu.CompilerParams(
                collective_id=0, has_side_effects=True,
                vmem_limit_bytes=48 * 1024 * 1024),
        )(q_in, k_in, v_in)
        out, lse = pl.pallas_call(
            store_kernel,
            out_shape=(jax.ShapeDtypeStruct(out.shape, BF16), jax.ShapeDtypeStruct(lse.shape, F32)),
            in_specs=[vmem, vmem],
            out_specs=(hbm, hbm),
            scratch_shapes=[pltpu.SemaphoreType.DMA((q_heads + 1,))],
            compiler_params=pltpu.CompilerParams(vmem_limit_bytes=48 * 1024 * 1024),
        )(out, lse)
        out_tok = out.reshape(q_heads, tok_count, head_dim).transpose(1, 0, 2)
        return out_tok, lse.T

    return jax.shard_map(local_attention, mesh=mesh, in_specs=(row_spec, row_spec, row_spec),
                         out_specs=(row_spec, lse_spec), check_vma=False)
```

```python
import functools
import math

import jax
import jax.numpy as jnp
from jax import lax
from jax.experimental import pallas as pl
from jax.experimental.pallas import tpu as pltpu
from jax.sharding import PartitionSpec as P

MESH = pl.DeviceIdType.MESH
F32 = jnp.float32
BF16 = jnp.bfloat16
UP, DOWN = 0, 1
LANES = 256
DEPTH = 3
DRAIN_LAG = 2
LAG_UP, LAG_DOWN = -2, 4
SOLO = 4


def attention_kernel(n_cp, q_hbm, k_hbm, v_hbm, o_ref, lse_ref, q_ref, kv_buf, raw_ref, wide_ref, acc_ref, max_ref,
                     sum_ref, send_sem, recv_sem, pair_send, pair_recv, own_sem, ready_sem):
    n_z = n_cp // 2
    kv_heads, _, _, half_len, head_dim = kv_buf.shape[2:]
    n_base = (n_z - 2) * kv_heads
    n_item = n_base + 2 * kv_heads
    group = q_ref.shape[0] // kv_heads
    rows = group * half_len
    scale = head_dim ** -0.5
    coef = scale * math.log2(math.e)
    me = lax.axis_index("cp")
    z, core = me // 2, me % 2
    way = core
    above = lax.rem(z + 1, n_z) * 2 + core
    below = lax.rem(z + n_z - 1, n_z) * 2 + core
    ahead_id = jnp.where(way == UP, above, below)
    behind_id = jnp.where(way == UP, below, above)
    partner = z * 2 + 1 - core
    z_next = ahead_id // 2

    raw_copies = [pltpu.make_async_copy(src, raw_ref.at[which], own_sem.at[which])
                  for which, src in enumerate((k_hbm, v_hbm))]
    for copy in raw_copies:
        copy.start()
    barrier = pltpu.get_barrier_semaphore()
    wraps_down = (z == 0) & (way == DOWN)
    before_wrap = (z == n_z - 1) & (way == DOWN)
    pl.semaphore_signal(barrier, inc=1, device_id={"cp": partner}, device_id_type=MESH)
    greeted = jnp.where(wraps_down, 1, jnp.where(before_wrap, 3, 2))

    @pl.when(jnp.logical_not(before_wrap))
    def _():
        pl.semaphore_signal(barrier, inc=1, device_id={"cp": behind_id}, device_id_type=MESH)

    @pl.when(wraps_down)
    def _():
        pl.semaphore_signal(barrier, inc=1, device_id={"cp": ahead_id}, device_id_type=MESH)

    q_copy = pltpu.make_async_copy(q_hbm, q_ref, own_sem.at[2])
    q_copy.start()

    def far_rings(chip_to):
        return jnp.where(chip_to == 0, DOWN, UP), jnp.where(chip_to <= 1, DOWN, UP)

    def far_early(ring, chip_to):
        shared = jnp.where(ring == UP, 1, kv_heads)
        return jnp.where(chip_to == 0, shared, jnp.where(ring == far_rings(chip_to)[0], kv_heads, 0))

    def halved(item, ring, chip_to):
        return (chip_to == 0) & (item == n_base + jnp.where(ring == UP, 0, kv_heads - 1))

    def place(item, ring):
        rnd = item // kv_heads
        extra = item - n_base
        far_part = jnp.where(extra < far_early(ring, z), 0, 1)
        far = item >= n_base
        chip = lax.rem(z + n_z + (2 * ring - 1) * (rnd // 2 + 1), n_z)
        far_chip = lax.rem(z + n_z // 2, n_z)
        head = jnp.where(far & (z == 0) & (ring == UP), kv_heads - 1, item % kv_heads)
        return jnp.where(far, far_part, rnd % 2), jnp.where(far, far_chip, chip), head

    def sized(place_of, half, side, act):
        @pl.when(half)
        def _():
            act(kv_buf.at[(*place_of, side)])

        @pl.when(jnp.logical_not(half))
        def _():
            act(kv_buf.at[place_of])

    def travels(item, ring, chip_to):
        step = item // kv_heads // 2 + 1
        extra = item - n_base
        early = far_early(ring, chip_to)
        source = lax.rem(chip_to + n_z - step, n_z)
        near = jnp.where(ring == UP, source > n_z // 2, chip_to + step < n_z)
        far = (ring == far_rings(chip_to)[1]) & (chip_to < n_z // 2) & (extra < early + kv_heads)
        return jnp.where(extra < 0, ((item // kv_heads) % 2 == 0) | near, (extra < early) | far)

    def useful(item, ring):
        part, chip, _ = place(item, ring)
        return travels(item, ring, z) & ((part == 0) | (chip > z))

    def ring_copy(block, item):
        return pltpu.make_async_remote_copy(
            src_ref=block, dst_ref=block, send_sem=send_sem.at[item], recv_sem=recv_sem.at[item],
            device_id={"cp": ahead_id}, device_id_type=MESH)

    def pair_copy(block, item):
        return pltpu.make_async_remote_copy(
            src_ref=block, dst_ref=block, send_sem=pair_send.at[item], recv_sem=pair_recv.at[item],
            device_id={"cp": partner}, device_id_type=MESH)

    acc_ref[...] = jnp.zeros_like(acc_ref)
    max_ref[...] = jnp.full_like(max_ref, -jnp.inf)
    sum_ref[...] = jnp.zeros_like(sum_ref)

    for copy in raw_copies:
        copy.wait()

    def split_heads(part):
        span = pl.ds(part * kv_heads * half_len, kv_heads * half_len)
        wide_ref[:, span] = raw_ref[:, span].astype(F32)
        for head in range(kv_heads):
            for which in range(2):
                start = part * kv_heads * half_len + head
                picked = wide_ref[which, pl.ds(start, half_len, stride=kv_heads), :]
                kv_buf[part, z, head, core, which] = picked.astype(BF16)

    def send_own(part, side):
        @pl.when(travels(part * kv_heads, way, z_next) & jnp.logical_not(wraps_down))
        def _():
            for head in range(kv_heads):
                ring_copy(kv_buf.at[part, z, head, side], part * kv_heads + head).start()

    for part in range(2):
        split_heads(part)
        if part == 0:
            pl.semaphore_wait(barrier, greeted)

            @pl.when(before_wrap)
            def _():
                pl.semaphore_signal(ready_sem, inc=1, device_id={"cp": behind_id}, device_id_type=MESH)

        for head in range(kv_heads):
            pair_copy(kv_buf.at[part, z, head, core], n_item + part * kv_heads + head).start()
        if part == 0:
            send_own(part, core)

    for part in range(2):
        if part > 0:
            send_own(part, core)
        for head in range(kv_heads):
            pair_copy(kv_buf.at[part, z, head, 1 - core], n_item + part * kv_heads + head).wait_recv()
        send_own(part, 1 - core)

    cuts = [(start, min(LANES, rows - start)) for start in range(0, rows, LANES)]

    def run_jobs(jobs, mask=None):
        tiles = [(job, start, size) for start, size in cuts for job in jobs]

        def keys(job, which):
            chip, part, _, head = job
            return kv_buf[part, chip, head, :, which].reshape(2 * half_len, head_dim)

        def scores(tile):
            job, start, size = tile
            _, _, half, head = job
            q_all = q_ref[pl.ds(head * group, group), half].reshape(rows, head_dim)
            s = lax.dot_general(keys(job, 0), q_all[start:start + size], (((1,), (1,)), ((), ())),
                                preferred_element_type=F32)
            if mask is not None:
                key_pos, query_base = mask
                lane = lax.broadcasted_iota(jnp.int32, (1, size), 1) + start
                s = jnp.where(key_pos <= query_base + lane % half_len, s, -jnp.inf)
            return s

        ahead = [scores(tile) for tile in tiles[:DEPTH]]
        for n, (job, start, size) in enumerate(tiles):
            _, _, half, head = job
            s = ahead.pop(0)
            if n + DEPTH < len(tiles):
                ahead.append(scores(tiles[n + DEPTH]))
            cols = slice(start, start + size)
            v_t = keys(job, 1).T
            old = max_ref[half, head, :, cols]
            new = jnp.maximum(old, jnp.max(s, axis=0, keepdims=True))
            p = jnp.exp2((s - new) * coef)
            alpha = jnp.exp2((old - new) * coef)
            max_ref[half, head, :, cols] = new
            part_sum = jnp.sum(p.reshape(-1, 8, size), axis=0)
            sum_ref[half, head, :, cols] = sum_ref[half, head, :, cols] * alpha + part_sum
            acc_ref[half, head, :, cols] = acc_ref[half, head, :, cols] * alpha + jnp.dot(
                v_t, p.astype(BF16), preferred_element_type=F32)

    def finish(half, heads):
        for head in heads:
            total = jnp.sum(sum_ref[half, head], axis=0, keepdims=True)
            lse = max_ref[half, head] * scale + jnp.log(total)
            inverse = 1.0 / total
            for g in range(group):
                lse_ref[head * group + g, half * half_len:(half + 1) * half_len] = (
                    lse[0, g * half_len:(g + 1) * half_len])
            out = (acc_ref[half, head] * inverse).astype(BF16).T
            o_ref[head * group:(head + 1) * group, half] = out.reshape(group, half_len, head_dim)

    q_copy.wait()

    row_id = lax.broadcasted_iota(jnp.int32, (2 * half_len, 1), 0)

    def own_masked(item, carry):
        part, head = item // kv_heads, item % kv_heads
        first_block = jnp.where(part == 0, 2 * z, 2 * n_cp - 1 - 2 * z)
        shift = jnp.where(part == 0, 0, 2 * half_len)
        key_pos = first_block * half_len + row_id - jnp.where(row_id >= half_len, shift, 0)
        query_block = jnp.where(part == 0, me, 2 * n_cp - 1 - me)
        run_jobs([(z, part, part, head)], (key_pos, query_block * half_len))
        return carry

    lax.fori_loop(0, 2 * kv_heads, own_masked, 0)

    @pl.when(wraps_down)
    def _():
        pl.semaphore_wait(ready_sem, 1)
        for head in range(kv_heads):
            ring_copy(kv_buf.at[0, z, head], head).start()


    def arrive(item):
        spot = place(item, way)
        part, _, head = spot
        sized(spot, halved(item, way, z), way, lambda block: ring_copy(block, item).wait_recv())
        final = item >= n_base - 2 * kv_heads
        early_ring, late_ring = far_rings(z_next)
        shift = jnp.where((z_next == 0) & (way == UP), kv_heads - 1, 0)
        far = n_base + head + jnp.where(part == 0, -shift, far_early(way, z_next))
        onward = jnp.where(final, far, item + 2 * kv_heads)
        early_goes = jnp.where(z_next == 0, head >= shift, way == early_ring)
        chosen = jnp.where(part == 0, early_goes, way == late_ring)

        @pl.when((item < n_base) & (jnp.logical_not(final) | chosen) & travels(onward, way, z_next))
        def _():
            sized(spot, halved(onward, way, z_next), way, lambda block: ring_copy(block, onward).start())

        @pl.when(useful(item, way))
        def _():
            sized(spot, halved(item, way, z), way, lambda block: pair_copy(block, item).start())

    def pair_arrive(item):
        sized(place(item, 1 - way), halved(item, 1 - way, z), 1 - way,
              lambda block: pair_copy(block, item).wait_recv())

    def job_of(item, ring):
        part, chip, head = place(jnp.maximum(item, 0), ring)
        lower = jnp.where(chip < z, 1, 0)
        remote = (chip, part * (1 - lower), 1 - part * lower, head)
        opening = (z, 0, 1, -1 - item)
        return tuple(jnp.where(item >= 0, b, a) for a, b in zip(opening, remote))

    def count(ring):
        return n_base + far_early(ring, z) + jnp.where(ring == far_rings(z)[1], kv_heads, 0)

    early_up = (z == 0) & (way == UP)
    lag = jnp.where(z == 0, jnp.where(way == UP, LAG_UP, LAG_DOWN), 1)

    def drain(item):
        block = kv_buf.at[0, z, 0]

        @pl.when(travels(item, way, z_next))
        def _():
            sized((0, z, 0), halved(item, way, z_next), way, lambda block: ring_copy(block, item).wait_send())

        @pl.when(useful(item, way))
        def _():
            sized((0, z, 0), halved(item, way, z), way, lambda block: pair_copy(block, item).wait_send())

    def remote_step(turn, carry):
        tick = turn - 4

        def fetch(item, ring, mine):
            @pl.when(mine & travels(item, ring, z))
            def _():
                arrive(item)

            @pl.when(jnp.logical_not(mine) & (item >= 0) & useful(item, ring))
            def _():
                pair_arrive(item)

        def valid(item, ring, first):
            return (item >= first) & (item < count(ring))

        def jobless(item, ring):
            return (ring == DOWN) & halved(item, ring, z)

        apart = jobless(tick, way) | jobless(tick - lag, 1 - way) | ((z == 0) & (tick >= n_base + SOLO))
        both = valid(tick, way, 0) & valid(tick - lag, 1 - way, -kv_heads) & jnp.logical_not(apart)

        @pl.when(both)
        def _():
            @pl.when(travels(tick, way, z))
            def _():
                arrive(tick)

            @pl.when((tick >= lag) & useful(tick - lag, 1 - way))
            def _():
                pair_arrive(tick - lag)

            run_jobs([job_of(tick, way), job_of(tick - lag, 1 - way)])

        def slot(which, inner):
            mine = which == jnp.where(early_up, 1, 0)
            item = jnp.where(mine, tick, tick - lag)
            ring = jnp.where(mine, way, 1 - way)

            @pl.when(valid(item, ring, jnp.where(mine, 0, -kv_heads)))
            def _():
                fetch(item, ring, mine)

                @pl.when(jnp.logical_not(jobless(item, ring)))
                def _():
                    run_jobs([job_of(item, ring)])

            return inner

        @pl.when(jnp.logical_not(both))
        def _():
            lax.fori_loop(0, 2, slot, 0)

        @pl.when(tick == 2 * kv_heads * z)
        def _():
            finish(0, range(kv_heads))

        @pl.when(z == 0)
        def _():
            @pl.when(tick == n_base + 2 + jnp.where(way == UP, lag, 0))
            def _():
                finish(1, range(1))

        done = tick - DRAIN_LAG

        @pl.when((done >= 0) & (done < n_item - 2))
        def _():
            drain(done)
        return carry

    lax.fori_loop(0, n_item + 5, remote_step, 0)

    @pl.when(z >= n_z // 2)
    def _():
        finish(0, range(kv_heads))

    @pl.when(z > 0)
    def _():
        finish(1, range(1))

    finish(1, range(1, kv_heads))

    for item in range(n_item - 2, n_item):
        drain(item)
    for item in range(2 * kv_heads):
        pair_copy(kv_buf.at[0, z, 0, core], n_item + item).wait_send()


def store_kernel(o_ref, lse_ref, o_hbm, lse_hbm, sems):
    copies = [pltpu.make_async_copy(o_ref, o_hbm, sems.at[0]), pltpu.make_async_copy(lse_ref, lse_hbm, sems.at[1])]
    for copy in copies:
        copy.start()
    for copy in copies:
        copy.wait()


def solution(mesh):
    n_cp = mesh.shape["cp"]
    row_spec = P(("dp", "cp"), None, None)
    lse_spec = P(("dp", "cp"), None)

    def local_attention(q_tok, k_tok, v_tok):
        tok_count, q_heads, head_dim = q_tok.shape
        kv_heads = k_tok.shape[1]
        group = q_heads // kv_heads
        half_len = tok_count // 2
        rows = group * half_len
        n_item = n_cp // 2 * kv_heads
        q_in = q_tok.transpose(1, 0, 2).reshape(q_heads, 2, half_len, head_dim)
        k_in = k_tok.reshape(tok_count * kv_heads, head_dim)
        v_in = v_tok.reshape(tok_count * kv_heads, head_dim)
        q_in, k_in, v_in = (pltpu.with_memory_space_constraint(x, pltpu.HBM) for x in (q_in, k_in, v_in))
        vmem = pl.BlockSpec(memory_space=pltpu.VMEM)
        hbm = pl.BlockSpec(memory_space=pltpu.HBM)
        out, lse = pl.pallas_call(
            functools.partial(attention_kernel, n_cp),
            out_shape=(pltpu.VMEM(q_in.shape, BF16), pltpu.VMEM((q_heads, tok_count), F32)),
            in_specs=[hbm, hbm, hbm],
            out_specs=(vmem, vmem),
            scratch_shapes=[
                pltpu.VMEM(q_in.shape, BF16),
                pltpu.VMEM((2, n_cp // 2, kv_heads, 2, 2, half_len, head_dim), BF16),
                pltpu.VMEM((2, tok_count * kv_heads, head_dim), BF16),
                pltpu.VMEM((2, tok_count * kv_heads, head_dim), F32),
                pltpu.VMEM((2, kv_heads, head_dim, rows), F32),
                pltpu.VMEM((2, kv_heads, 1, rows), F32),
                pltpu.VMEM((2, kv_heads, 8, rows), F32),
                pltpu.SemaphoreType.DMA((n_item,)),
                pltpu.SemaphoreType.DMA((n_item,)),
                pltpu.SemaphoreType.DMA((n_item + 2 * kv_heads,)),
                pltpu.SemaphoreType.DMA((n_item + 2 * kv_heads,)),
                pltpu.SemaphoreType.DMA((3,)),
                pltpu.SemaphoreType.REGULAR,
            ],
            compiler_params=pltpu.CompilerParams(
                collective_id=0, has_side_effects=True,
                vmem_limit_bytes=48 * 1024 * 1024),
        )(q_in, k_in, v_in)
        out, lse = pl.pallas_call(
            store_kernel,
            out_shape=(jax.ShapeDtypeStruct(out.shape, BF16), jax.ShapeDtypeStruct(lse.shape, F32)),
            in_specs=[vmem, vmem],
            out_specs=(hbm, hbm),
            scratch_shapes=[pltpu.SemaphoreType.DMA((2,))],
            compiler_params=pltpu.CompilerParams(vmem_limit_bytes=48 * 1024 * 1024),
        )(out, lse)
        out_tok = out.reshape(q_heads, tok_count, head_dim).transpose(1, 0, 2)
        return out_tok, lse.T

    return jax.shard_map(local_attention, mesh=mesh, in_specs=(row_spec, row_spec, row_spec),
                         out_specs=(row_spec, lse_spec), check_vma=False)
```

```python
import functools
import math

import jax
import jax.numpy as jnp
from jax import lax
from jax.experimental import pallas as pl
from jax.experimental.pallas import tpu as pltpu
from jax.sharding import PartitionSpec as P

MESH = pl.DeviceIdType.MESH
F32 = jnp.float32
BF16 = jnp.bfloat16
UP, DOWN = 0, 1
LANES = 256
DEPTH = 3
DRAIN_LAG = 2
LAG_UP, LAG_DOWN = -2, 4
SOLO = 4


def attention_kernel(n_cp, q_hbm, k_hbm, v_hbm, o_ref, lse_ref, q_ref, kv_buf, raw_ref, wide_ref, acc_ref, max_ref,
                     sum_ref, send_sem, recv_sem, pair_send, pair_recv, own_sem, ready_sem):
    n_z = n_cp // 2
    kv_heads, _, _, half_len, head_dim = kv_buf.shape[2:]
    n_base = (n_z - 2) * kv_heads
    n_item = n_base + 2 * kv_heads
    group = q_ref.shape[0] // kv_heads
    rows = group * half_len
    scale = head_dim ** -0.5
    coef = scale * math.log2(math.e)
    me = lax.axis_index("cp")
    z, core = me // 2, me % 2
    way = core
    above = lax.rem(z + 1, n_z) * 2 + core
    below = lax.rem(z + n_z - 1, n_z) * 2 + core
    ahead_id = jnp.where(way == UP, above, below)
    behind_id = jnp.where(way == UP, below, above)
    partner = z * 2 + 1 - core
    z_next = ahead_id // 2

    raw_copies = [pltpu.make_async_copy(src, raw_ref.at[which], own_sem.at[which])
                  for which, src in enumerate((k_hbm, v_hbm))]
    for copy in raw_copies:
        copy.start()
    barrier = pltpu.get_barrier_semaphore()
    wraps_down = (z == 0) & (way == DOWN)
    before_wrap = (z == n_z - 1) & (way == DOWN)
    pl.semaphore_signal(barrier, inc=1, device_id={"cp": partner}, device_id_type=MESH)
    greeted = jnp.where(wraps_down, 1, jnp.where(before_wrap, 3, 2))

    @pl.when(jnp.logical_not(before_wrap))
    def _():
        pl.semaphore_signal(barrier, inc=1, device_id={"cp": behind_id}, device_id_type=MESH)

    @pl.when(wraps_down)
    def _():
        pl.semaphore_signal(barrier, inc=1, device_id={"cp": ahead_id}, device_id_type=MESH)

    q_copy = pltpu.make_async_copy(q_hbm, q_ref, own_sem.at[2])
    q_copy.start()

    def far_rings(chip_to):
        return jnp.where(chip_to == 0, DOWN, UP), jnp.where(chip_to <= 1, DOWN, UP)

    def far_early(ring, chip_to):
        shared = jnp.where(ring == UP, 1, kv_heads)
        return jnp.where(chip_to == 0, shared, jnp.where(ring == far_rings(chip_to)[0], kv_heads, 0))

    def halved(item, ring, chip_to):
        return (chip_to == 0) & (item == n_base + jnp.where(ring == UP, 0, kv_heads - 1))

    def place(item, ring):
        rnd = item // kv_heads
        extra = item - n_base
        far_part = jnp.where(extra < far_early(ring, z), 0, 1)
        far = item >= n_base
        chip = lax.rem(z + n_z + (2 * ring - 1) * (rnd // 2 + 1), n_z)
        far_chip = lax.rem(z + n_z // 2, n_z)
        head = jnp.where(far & (z == 0) & (ring == UP), kv_heads - 1, item % kv_heads)
        return jnp.where(far, far_part, rnd % 2), jnp.where(far, far_chip, chip), head

    def sized(place_of, half, side, act):
        @pl.when(half)
        def _():
            act(kv_buf.at[(*place_of, side)])

        @pl.when(jnp.logical_not(half))
        def _():
            act(kv_buf.at[place_of])

    def travels(item, ring, chip_to):
        step = item // kv_heads // 2 + 1
        extra = item - n_base
        early = far_early(ring, chip_to)
        source = lax.rem(chip_to + n_z - step, n_z)
        near = jnp.where(ring == UP, source > n_z // 2, chip_to + step < n_z)
        far = (ring == far_rings(chip_to)[1]) & (chip_to < n_z // 2) & (extra < early + kv_heads)
        return jnp.where(extra < 0, ((item // kv_heads) % 2 == 0) | near, (extra < early) | far)

    def useful(item, ring):
        part, chip, _ = place(item, ring)
        return travels(item, ring, z) & ((part == 0) | (chip > z))

    def ring_copy(block, item):
        return pltpu.make_async_remote_copy(
            src_ref=block, dst_ref=block, send_sem=send_sem.at[item], recv_sem=recv_sem.at[item],
            device_id={"cp": ahead_id}, device_id_type=MESH)

    def pair_copy(block, item):
        return pltpu.make_async_remote_copy(
            src_ref=block, dst_ref=block, send_sem=pair_send.at[item], recv_sem=pair_recv.at[item],
            device_id={"cp": partner}, device_id_type=MESH)

    acc_ref[...] = jnp.zeros_like(acc_ref)
    max_ref[...] = jnp.full_like(max_ref, -jnp.inf)
    sum_ref[...] = jnp.zeros_like(sum_ref)

    for copy in raw_copies:
        copy.wait()

    def split_heads(part):
        span = pl.ds(part * kv_heads * half_len, kv_heads * half_len)
        wide_ref[:, span] = raw_ref[:, span].astype(F32)
        for head in range(kv_heads):
            for which in range(2):
                start = part * kv_heads * half_len + head
                picked = wide_ref[which, pl.ds(start, half_len, stride=kv_heads), :]
                kv_buf[part, z, head, core, which] = picked.astype(BF16)

    def send_own(part, side):
        @pl.when(travels(part * kv_heads, way, z_next) & jnp.logical_not(wraps_down))
        def _():
            for head in range(kv_heads):
                ring_copy(kv_buf.at[part, z, head, side], part * kv_heads + head).start()

    for part in range(2):
        split_heads(part)
        if part == 0:
            pl.semaphore_wait(barrier, greeted)

            @pl.when(before_wrap)
            def _():
                pl.semaphore_signal(ready_sem, inc=1, device_id={"cp": behind_id}, device_id_type=MESH)

        for head in range(kv_heads):
            pair_copy(kv_buf.at[part, z, head, core], n_item + part * kv_heads + head).start()
        if part == 0:
            send_own(part, core)

    for part in range(2):
        if part > 0:
            send_own(part, core)
        for head in range(kv_heads):
            pair_copy(kv_buf.at[part, z, head, 1 - core], n_item + part * kv_heads + head).wait_recv()
        send_own(part, 1 - core)

    cuts = [(start, min(LANES, rows - start)) for start in range(0, rows, LANES)]

    def run_jobs(jobs, mask=None, side=None):
        tiles = [(job, start, size) for start, size in cuts for job in jobs]

        def keys(job, which):
            chip, part, _, head = job
            if side is not None:
                return kv_buf[part, chip, head, side, which]
            return kv_buf[part, chip, head, :, which].reshape(2 * half_len, head_dim)

        def scores(tile):
            job, start, size = tile
            _, _, half, head = job
            q_all = q_ref[pl.ds(head * group, group), half].reshape(rows, head_dim)
            s = lax.dot_general(keys(job, 0), q_all[start:start + size], (((1,), (1,)), ((), ())),
                                preferred_element_type=F32)
            if mask is not None:
                key_pos, query_base = mask
                lane = lax.broadcasted_iota(jnp.int32, (1, size), 1) + start
                s = jnp.where(key_pos <= query_base + lane % half_len, s, -jnp.inf)
            return s

        ahead = [scores(tile) for tile in tiles[:DEPTH]]
        for n, (job, start, size) in enumerate(tiles):
            _, _, half, head = job
            s = ahead.pop(0)
            if n + DEPTH < len(tiles):
                ahead.append(scores(tiles[n + DEPTH]))
            cols = slice(start, start + size)
            v_t = keys(job, 1).T
            old = max_ref[half, head, :, cols]
            new = jnp.maximum(old, jnp.max(s, axis=0, keepdims=True))
            p = jnp.exp2((s - new) * coef)
            alpha = jnp.exp2((old - new) * coef)
            max_ref[half, head, :, cols] = new
            part_sum = jnp.sum(p.reshape(-1, 8, size), axis=0)
            sum_ref[half, head, :, cols] = sum_ref[half, head, :, cols] * alpha + part_sum
            acc_ref[half, head, :, cols] = acc_ref[half, head, :, cols] * alpha + jnp.dot(
                v_t, p.astype(BF16), preferred_element_type=F32)

    def finish(half, heads):
        for head in heads:
            total = jnp.sum(sum_ref[half, head], axis=0, keepdims=True)
            lse = max_ref[half, head] * scale + jnp.log(total)
            inverse = 1.0 / total
            for g in range(group):
                lse_ref[head * group + g, half * half_len:(half + 1) * half_len] = (
                    lse[0, g * half_len:(g + 1) * half_len])
            out = (acc_ref[half, head] * inverse).astype(BF16).T
            o_ref[head * group:(head + 1) * group, half] = out.reshape(group, half_len, head_dim)

    q_copy.wait()

    row_id = lax.broadcasted_iota(jnp.int32, (2 * half_len, 1), 0)

    def own_masked(item, carry):
        part, head = item // kv_heads, item % kv_heads
        first_block = jnp.where(part == 0, 2 * z, 2 * n_cp - 1 - 2 * z)
        shift = jnp.where(part == 0, 0, 2 * half_len)
        key_pos = first_block * half_len + row_id - jnp.where(row_id >= half_len, shift, 0)
        query_block = jnp.where(part == 0, me, 2 * n_cp - 1 - me)
        run_jobs([(z, part, part, head)], (key_pos, query_block * half_len))
        return carry

    lax.fori_loop(0, 2 * kv_heads, own_masked, 0)

    @pl.when(wraps_down)
    def _():
        pl.semaphore_wait(ready_sem, 1)
        for head in range(kv_heads):
            ring_copy(kv_buf.at[0, z, head], head).start()


    def arrive(item):
        spot = place(item, way)
        part, _, head = spot
        sized(spot, halved(item, way, z), way, lambda block: ring_copy(block, item).wait_recv())
        final = item >= n_base - 2 * kv_heads
        early_ring, late_ring = far_rings(z_next)
        shift = jnp.where((z_next == 0) & (way == UP), kv_heads - 1, 0)
        far = n_base + head + jnp.where(part == 0, -shift, far_early(way, z_next))
        onward = jnp.where(final, far, item + 2 * kv_heads)
        early_goes = jnp.where(z_next == 0, head >= shift, way == early_ring)
        chosen = jnp.where(part == 0, early_goes, way == late_ring)

        @pl.when((item < n_base) & (jnp.logical_not(final) | chosen) & travels(onward, way, z_next))
        def _():
            sized(spot, halved(onward, way, z_next), way, lambda block: ring_copy(block, onward).start())

        @pl.when(useful(item, way))
        def _():
            sized(spot, halved(item, way, z), way, lambda block: pair_copy(block, item).start())

    def pair_arrive(item):
        sized(place(item, 1 - way), halved(item, 1 - way, z), 1 - way,
              lambda block: pair_copy(block, item).wait_recv())

    def job_of(item, ring):
        part, chip, head = place(jnp.maximum(item, 0), ring)
        lower = jnp.where(chip < z, 1, 0)
        remote = (chip, part * (1 - lower), 1 - part * lower, head)
        opening = (z, 0, 1, -1 - item)
        return tuple(jnp.where(item >= 0, b, a) for a, b in zip(opening, remote))

    def count(ring):
        return n_base + far_early(ring, z) + jnp.where(ring == far_rings(z)[1], kv_heads, 0)

    early_up = (z == 0) & (way == UP)
    lag = jnp.where(z == 0, jnp.where(way == UP, LAG_UP, LAG_DOWN), 1)

    def drain(item):
        block = kv_buf.at[0, z, 0]

        @pl.when(travels(item, way, z_next))
        def _():
            sized((0, z, 0), halved(item, way, z_next), way, lambda block: ring_copy(block, item).wait_send())

        @pl.when(useful(item, way))
        def _():
            sized((0, z, 0), halved(item, way, z), way, lambda block: pair_copy(block, item).wait_send())

    def remote_step(turn, carry):
        tick = turn - 4

        def fetch(item, ring, mine):
            @pl.when(mine & travels(item, ring, z))
            def _():
                arrive(item)

            @pl.when(jnp.logical_not(mine) & (item >= 0) & useful(item, ring))
            def _():
                pair_arrive(item)

        def valid(item, ring, first):
            return (item >= first) & (item < count(ring))

        apart = halved(tick, way, z) | halved(tick - lag, 1 - way, z) | ((z == 0) & (tick >= n_base + SOLO))
        both = valid(tick, way, 0) & valid(tick - lag, 1 - way, -kv_heads) & jnp.logical_not(apart)

        @pl.when(both)
        def _():
            @pl.when(travels(tick, way, z))
            def _():
                arrive(tick)

            @pl.when((tick >= lag) & useful(tick - lag, 1 - way))
            def _():
                pair_arrive(tick - lag)

            run_jobs([job_of(tick, way), job_of(tick - lag, 1 - way)])

        def slot(which, inner):
            mine = which == jnp.where(early_up, 1, 0)
            item = jnp.where(mine, tick, tick - lag)
            ring = jnp.where(mine, way, 1 - way)

            @pl.when(valid(item, ring, jnp.where(mine, 0, -kv_heads)))
            def _():
                fetch(item, ring, mine)

                half = halved(item, ring, z)

                @pl.when(half)
                def _():
                    run_jobs([job_of(item, ring)], side=ring)

                @pl.when(jnp.logical_not(half))
                def _():
                    run_jobs([job_of(item, ring)])

            return inner

        @pl.when(jnp.logical_not(both))
        def _():
            lax.fori_loop(0, 2, slot, 0)

        @pl.when(tick == 2 * kv_heads * z)
        def _():
            finish(0, range(kv_heads))

        @pl.when(z == 0)
        def _():
            @pl.when(tick == n_base + 2 + jnp.where(way == UP, lag, 0))
            def _():
                finish(1, range(1))

        done = tick - DRAIN_LAG

        @pl.when((done >= 0) & (done < n_item - 2))
        def _():
            drain(done)
        return carry

    lax.fori_loop(0, n_item + 5, remote_step, 0)

    @pl.when(z >= n_z // 2)
    def _():
        finish(0, range(kv_heads))

    @pl.when(z > 0)
    def _():
        finish(1, range(1))

    finish(1, range(1, kv_heads))

    for item in range(n_item - 2, n_item):
        drain(item)
    for item in range(2 * kv_heads):
        pair_copy(kv_buf.at[0, z, 0, core], n_item + item).wait_send()


def store_kernel(o_ref, lse_ref, o_hbm, lse_hbm, sems):
    copies = [pltpu.make_async_copy(o_ref, o_hbm, sems.at[0]), pltpu.make_async_copy(lse_ref, lse_hbm, sems.at[1])]
    for copy in copies:
        copy.start()
    for copy in copies:
        copy.wait()


def solution(mesh):
    n_cp = mesh.shape["cp"]
    row_spec = P(("dp", "cp"), None, None)
    lse_spec = P(("dp", "cp"), None)

    def local_attention(q_tok, k_tok, v_tok):
        tok_count, q_heads, head_dim = q_tok.shape
        kv_heads = k_tok.shape[1]
        group = q_heads // kv_heads
        half_len = tok_count // 2
        rows = group * half_len
        n_item = n_cp // 2 * kv_heads
        q_in = q_tok.transpose(1, 0, 2).reshape(q_heads, 2, half_len, head_dim)
        k_in = k_tok.reshape(tok_count * kv_heads, head_dim)
        v_in = v_tok.reshape(tok_count * kv_heads, head_dim)
        q_in, k_in, v_in = (pltpu.with_memory_space_constraint(x, pltpu.HBM) for x in (q_in, k_in, v_in))
        vmem = pl.BlockSpec(memory_space=pltpu.VMEM)
        hbm = pl.BlockSpec(memory_space=pltpu.HBM)
        out, lse = pl.pallas_call(
            functools.partial(attention_kernel, n_cp),
            out_shape=(pltpu.VMEM(q_in.shape, BF16), pltpu.VMEM((q_heads, tok_count), F32)),
            in_specs=[hbm, hbm, hbm],
            out_specs=(vmem, vmem),
            scratch_shapes=[
                pltpu.VMEM(q_in.shape, BF16),
                pltpu.VMEM((2, n_cp // 2, kv_heads, 2, 2, half_len, head_dim), BF16),
                pltpu.VMEM((2, tok_count * kv_heads, head_dim), BF16),
                pltpu.VMEM((2, tok_count * kv_heads, head_dim), F32),
                pltpu.VMEM((2, kv_heads, head_dim, rows), F32),
                pltpu.VMEM((2, kv_heads, 1, rows), F32),
                pltpu.VMEM((2, kv_heads, 8, rows), F32),
                pltpu.SemaphoreType.DMA((n_item,)),
                pltpu.SemaphoreType.DMA((n_item,)),
                pltpu.SemaphoreType.DMA((n_item + 2 * kv_heads,)),
                pltpu.SemaphoreType.DMA((n_item + 2 * kv_heads,)),
                pltpu.SemaphoreType.DMA((3,)),
                pltpu.SemaphoreType.REGULAR,
            ],
            compiler_params=pltpu.CompilerParams(
                collective_id=0, has_side_effects=True,
                vmem_limit_bytes=48 * 1024 * 1024),
        )(q_in, k_in, v_in)
        out, lse = pl.pallas_call(
            store_kernel,
            out_shape=(jax.ShapeDtypeStruct(out.shape, BF16), jax.ShapeDtypeStruct(lse.shape, F32)),
            in_specs=[vmem, vmem],
            out_specs=(hbm, hbm),
            scratch_shapes=[pltpu.SemaphoreType.DMA((2,))],
            compiler_params=pltpu.CompilerParams(vmem_limit_bytes=48 * 1024 * 1024),
        )(out, lse)
        out_tok = out.reshape(q_heads, tok_count, head_dim).transpose(1, 0, 2)
        return out_tok, lse.T

    return jax.shard_map(local_attention, mesh=mesh, in_specs=(row_spec, row_spec, row_spec),
                         out_specs=(row_spec, lse_spec), check_vma=False)
```

```python
import functools
import math

import jax
import jax.numpy as jnp
from jax import lax
from jax.experimental import pallas as pl
from jax.experimental.pallas import tpu as pltpu
from jax.sharding import PartitionSpec as P

MESH = pl.DeviceIdType.MESH
F32 = jnp.float32
BF16 = jnp.bfloat16
UP, DOWN = 0, 1
LANES = 256
DEPTH = 4
DRAIN_LAG = 2
LAG_UP, LAG_DOWN = -2, 4
SOLO = 4


def attention_kernel(n_cp, q_hbm, k_hbm, v_hbm, o_ref, lse_ref, q_ref, kv_buf, raw_ref, wide_ref, acc_ref, max_ref,
                     sum_ref, send_sem, recv_sem, pair_send, pair_recv, own_sem, ready_sem):
    n_z = n_cp // 2
    kv_heads, _, _, half_len, head_dim = kv_buf.shape[2:]
    n_base = (n_z - 2) * kv_heads
    n_item = n_base + 2 * kv_heads
    group = q_ref.shape[0] // kv_heads
    rows = group * half_len
    scale = head_dim ** -0.5
    coef = scale * math.log2(math.e)
    me = lax.axis_index("cp")
    z, core = me // 2, me % 2
    way = core
    above = lax.rem(z + 1, n_z) * 2 + core
    below = lax.rem(z + n_z - 1, n_z) * 2 + core
    ahead_id = jnp.where(way == UP, above, below)
    behind_id = jnp.where(way == UP, below, above)
    partner = z * 2 + 1 - core
    z_next = ahead_id // 2

    part_rows = kv_heads * half_len
    raw_copies = [[pltpu.make_async_copy(src.at[pl.ds(part * part_rows, part_rows)],
                                         raw_ref.at[which, pl.ds(part * part_rows, part_rows)],
                                         own_sem.at[3 + 2 * part + which])
                   for which, src in enumerate((k_hbm, v_hbm))] for part in range(2)]
    for copy in raw_copies[0] + raw_copies[1]:
        copy.start()
    barrier = pltpu.get_barrier_semaphore()
    wraps_down = (z == 0) & (way == DOWN)
    before_wrap = (z == n_z - 1) & (way == DOWN)
    pl.semaphore_signal(barrier, inc=1, device_id={"cp": partner}, device_id_type=MESH)
    greeted = jnp.where(wraps_down, 1, jnp.where(before_wrap, 3, 2))

    @pl.when(jnp.logical_not(before_wrap))
    def _():
        pl.semaphore_signal(barrier, inc=1, device_id={"cp": behind_id}, device_id_type=MESH)

    @pl.when(wraps_down)
    def _():
        pl.semaphore_signal(barrier, inc=1, device_id={"cp": ahead_id}, device_id_type=MESH)

    q_copy = pltpu.make_async_copy(q_hbm, q_ref, own_sem.at[2])
    q_copy.start()

    def far_rings(chip_to):
        return jnp.where(chip_to == 0, DOWN, UP), jnp.where(chip_to <= 1, DOWN, UP)

    def far_early(ring, chip_to):
        shared = jnp.where(ring == UP, 1, kv_heads)
        return jnp.where(chip_to == 0, shared, jnp.where(ring == far_rings(chip_to)[0], kv_heads, 0))

    def halved(item, ring, chip_to):
        return (chip_to == 0) & (item == n_base + jnp.where(ring == UP, 0, kv_heads - 1))

    def place(item, ring):
        rnd = item // kv_heads
        extra = item - n_base
        far_part = jnp.where(extra < far_early(ring, z), 0, 1)
        far = item >= n_base
        chip = lax.rem(z + n_z + (2 * ring - 1) * (rnd // 2 + 1), n_z)
        far_chip = lax.rem(z + n_z // 2, n_z)
        head = jnp.where(far & (z == 0) & (ring == UP), kv_heads - 1, item % kv_heads)
        return jnp.where(far, far_part, rnd % 2), jnp.where(far, far_chip, chip), head

    def sized(place_of, half, side, act):
        @pl.when(half)
        def _():
            act(kv_buf.at[(*place_of, side)])

        @pl.when(jnp.logical_not(half))
        def _():
            act(kv_buf.at[place_of])

    def travels(item, ring, chip_to):
        step = item // kv_heads // 2 + 1
        extra = item - n_base
        early = far_early(ring, chip_to)
        source = lax.rem(chip_to + n_z - step, n_z)
        near = jnp.where(ring == UP, source > n_z // 2, chip_to + step < n_z)
        far = (ring == far_rings(chip_to)[1]) & (chip_to < n_z // 2) & (extra < early + kv_heads)
        return jnp.where(extra < 0, ((item // kv_heads) % 2 == 0) | near, (extra < early) | far)

    def useful(item, ring):
        part, chip, _ = place(item, ring)
        return travels(item, ring, z) & ((part == 0) | (chip > z))

    def ring_copy(block, item):
        return pltpu.make_async_remote_copy(
            src_ref=block, dst_ref=block, send_sem=send_sem.at[item], recv_sem=recv_sem.at[item],
            device_id={"cp": ahead_id}, device_id_type=MESH)

    def pair_copy(block, item):
        return pltpu.make_async_remote_copy(
            src_ref=block, dst_ref=block, send_sem=pair_send.at[item], recv_sem=pair_recv.at[item],
            device_id={"cp": partner}, device_id_type=MESH)

    acc_ref[...] = jnp.zeros_like(acc_ref)
    max_ref[...] = jnp.full_like(max_ref, -jnp.inf)
    sum_ref[...] = jnp.zeros_like(sum_ref)


    def split_heads(part):
        span = pl.ds(part * kv_heads * half_len, kv_heads * half_len)
        wide_ref[:, span] = raw_ref[:, span].astype(F32)
        for head in range(kv_heads):
            for which in range(2):
                start = part * kv_heads * half_len + head
                picked = wide_ref[which, pl.ds(start, half_len, stride=kv_heads), :]
                kv_buf[part, z, head, core, which] = picked.astype(BF16)

    def send_own(part, side):
        @pl.when(travels(part * kv_heads, way, z_next) & jnp.logical_not(wraps_down))
        def _():
            for head in range(kv_heads):
                ring_copy(kv_buf.at[part, z, head, side], part * kv_heads + head).start()

    for part in range(2):
        for copy in raw_copies[part]:
            copy.wait()
        split_heads(part)
        if part == 0:
            pl.semaphore_wait(barrier, greeted)

            @pl.when(before_wrap)
            def _():
                pl.semaphore_signal(ready_sem, inc=1, device_id={"cp": behind_id}, device_id_type=MESH)

        for head in range(kv_heads):
            pair_copy(kv_buf.at[part, z, head, core], n_item + part * kv_heads + head).start()
        if part == 0:
            send_own(part, core)

    for part in range(2):
        if part > 0:
            send_own(part, core)
        for head in range(kv_heads):
            pair_copy(kv_buf.at[part, z, head, 1 - core], n_item + part * kv_heads + head).wait_recv()
        send_own(part, 1 - core)

    cuts = [(start, min(LANES, rows - start)) for start in range(0, rows, LANES)]

    def run_jobs(jobs, mask=None, side=None):
        tiles = [(job, start, size) for start, size in cuts for job in jobs]

        def keys(job, which):
            chip, part, _, head = job
            if side is not None:
                return kv_buf[part, chip, head, side, which]
            return kv_buf[part, chip, head, :, which].reshape(2 * half_len, head_dim)

        def scores(tile):
            job, start, size = tile
            _, _, half, head = job
            q_all = q_ref[pl.ds(head * group, group), half].reshape(rows, head_dim)
            s = lax.dot_general(keys(job, 0), q_all[start:start + size], (((1,), (1,)), ((), ())),
                                preferred_element_type=F32)
            if mask is not None:
                key_pos, query_base = mask
                lane = lax.broadcasted_iota(jnp.int32, (1, size), 1) + start
                s = jnp.where(key_pos <= query_base + lane % half_len, s, -jnp.inf)
            return s

        ahead = [scores(tile) for tile in tiles[:DEPTH]]
        for n, (job, start, size) in enumerate(tiles):
            _, _, half, head = job
            s = ahead.pop(0)
            if n + DEPTH < len(tiles):
                ahead.append(scores(tiles[n + DEPTH]))
            cols = slice(start, start + size)
            v_t = keys(job, 1).T
            old = max_ref[half, head, :, cols]
            new = jnp.maximum(old, jnp.max(s, axis=0, keepdims=True))
            p = jnp.exp2((s - new) * coef)
            alpha = jnp.exp2((old - new) * coef)
            max_ref[half, head, :, cols] = new
            part_sum = jnp.sum(p.reshape(-1, 8, size), axis=0)
            sum_ref[half, head, :, cols] = sum_ref[half, head, :, cols] * alpha + part_sum
            acc_ref[half, head, :, cols] = acc_ref[half, head, :, cols] * alpha + jnp.dot(
                v_t, p.astype(BF16), preferred_element_type=F32)

    def finish(half, heads):
        for head in heads:
            total = jnp.sum(sum_ref[half, head], axis=0, keepdims=True)
            lse = max_ref[half, head] * scale + jnp.log(total)
            inverse = 1.0 / total
            for g in range(group):
                lse_ref[head * group + g, half * half_len:(half + 1) * half_len] = (
                    lse[0, g * half_len:(g + 1) * half_len])
            out = (acc_ref[half, head] * inverse).astype(BF16).T
            o_ref[head * group:(head + 1) * group, half] = out.reshape(group, half_len, head_dim)

    q_copy.wait()

    row_id = lax.broadcasted_iota(jnp.int32, (2 * half_len, 1), 0)

    def own_masked(item, carry):
        part, head = item // kv_heads, item % kv_heads
        first_block = jnp.where(part == 0, 2 * z, 2 * n_cp - 1 - 2 * z)
        shift = jnp.where(part == 0, 0, 2 * half_len)
        key_pos = first_block * half_len + row_id - jnp.where(row_id >= half_len, shift, 0)
        query_block = jnp.where(part == 0, me, 2 * n_cp - 1 - me)
        run_jobs([(z, part, part, head)], (key_pos, query_block * half_len))
        return carry

    lax.fori_loop(0, 2 * kv_heads, own_masked, 0)

    @pl.when(wraps_down)
    def _():
        pl.semaphore_wait(ready_sem, 1)
        for head in range(kv_heads):
            ring_copy(kv_buf.at[0, z, head], head).start()


    def arrive(item):
        spot = place(item, way)
        part, _, head = spot
        sized(spot, halved(item, way, z), way, lambda block: ring_copy(block, item).wait_recv())
        final = item >= n_base - 2 * kv_heads
        early_ring, late_ring = far_rings(z_next)
        shift = jnp.where((z_next == 0) & (way == UP), kv_heads - 1, 0)
        far = n_base + head + jnp.where(part == 0, -shift, far_early(way, z_next))
        onward = jnp.where(final, far, item + 2 * kv_heads)
        early_goes = jnp.where(z_next == 0, head >= shift, way == early_ring)
        chosen = jnp.where(part == 0, early_goes, way == late_ring)

        @pl.when((item < n_base) & (jnp.logical_not(final) | chosen) & travels(onward, way, z_next))
        def _():
            sized(spot, halved(onward, way, z_next), way, lambda block: ring_copy(block, onward).start())

        @pl.when(useful(item, way))
        def _():
            sized(spot, halved(item, way, z), way, lambda block: pair_copy(block, item).start())

    def pair_arrive(item):
        sized(place(item, 1 - way), halved(item, 1 - way, z), 1 - way,
              lambda block: pair_copy(block, item).wait_recv())

    def job_of(item, ring):
        part, chip, head = place(jnp.maximum(item, 0), ring)
        lower = jnp.where(chip < z, 1, 0)
        remote = (chip, part * (1 - lower), 1 - part * lower, head)
        opening = (z, 0, 1, -1 - item)
        return tuple(jnp.where(item >= 0, b, a) for a, b in zip(opening, remote))

    def count(ring):
        return n_base + far_early(ring, z) + jnp.where(ring == far_rings(z)[1], kv_heads, 0)

    early_up = (z == 0) & (way == UP)
    lag = jnp.where(z == 0, jnp.where(way == UP, LAG_UP, LAG_DOWN), 1)

    def drain(item):
        block = kv_buf.at[0, z, 0]

        @pl.when(travels(item, way, z_next))
        def _():
            sized((0, z, 0), halved(item, way, z_next), way, lambda block: ring_copy(block, item).wait_send())

        @pl.when(useful(item, way))
        def _():
            sized((0, z, 0), halved(item, way, z), way, lambda block: pair_copy(block, item).wait_send())

    def remote_step(turn, carry):
        tick = turn - 4

        def fetch(item, ring, mine):
            @pl.when(mine & travels(item, ring, z))
            def _():
                arrive(item)

            @pl.when(jnp.logical_not(mine) & (item >= 0) & useful(item, ring))
            def _():
                pair_arrive(item)

        def valid(item, ring, first):
            return (item >= first) & (item < count(ring))

        apart = halved(tick, way, z) | halved(tick - lag, 1 - way, z) | ((z == 0) & (tick >= n_base + SOLO))
        both = valid(tick, way, 0) & valid(tick - lag, 1 - way, -kv_heads) & jnp.logical_not(apart)

        @pl.when(both)
        def _():
            @pl.when(travels(tick, way, z))
            def _():
                arrive(tick)

            @pl.when((tick >= lag) & useful(tick - lag, 1 - way))
            def _():
                pair_arrive(tick - lag)

            run_jobs([job_of(tick, way), job_of(tick - lag, 1 - way)])

        def slot(which, inner):
            mine = which == jnp.where(early_up, 1, 0)
            item = jnp.where(mine, tick, tick - lag)
            ring = jnp.where(mine, way, 1 - way)

            @pl.when(valid(item, ring, jnp.where(mine, 0, -kv_heads)))
            def _():
                fetch(item, ring, mine)

                half = halved(item, ring, z)

                @pl.when(half)
                def _():
                    run_jobs([job_of(item, ring)], side=ring)

                @pl.when(jnp.logical_not(half))
                def _():
                    run_jobs([job_of(item, ring)])

            return inner

        @pl.when(jnp.logical_not(both))
        def _():
            lax.fori_loop(0, 2, slot, 0)

        @pl.when(tick == 2 * kv_heads * z)
        def _():
            finish(0, range(kv_heads))

        @pl.when(z == 0)
        def _():
            @pl.when(tick == n_base + 2 + jnp.where(way == UP, lag, 0))
            def _():
                finish(1, range(1))

        done = tick - DRAIN_LAG

        @pl.when((done >= 0) & (done < n_item - 2))
        def _():
            drain(done)
        return carry

    lax.fori_loop(0, n_item + 5, remote_step, 0)

    @pl.when(z >= n_z // 2)
    def _():
        finish(0, range(kv_heads))

    @pl.when(z > 0)
    def _():
        finish(1, range(1))

    finish(1, range(1, kv_heads))

    for item in range(n_item - 2, n_item):
        drain(item)
    for item in range(2 * kv_heads):
        pair_copy(kv_buf.at[0, z, 0, core], n_item + item).wait_send()


def store_kernel(o_ref, lse_ref, o_hbm, lse_hbm, sems):
    copies = [pltpu.make_async_copy(o_ref, o_hbm, sems.at[0]), pltpu.make_async_copy(lse_ref, lse_hbm, sems.at[1])]
    for copy in copies:
        copy.start()
    for copy in copies:
        copy.wait()


def solution(mesh):
    n_cp = mesh.shape["cp"]
    row_spec = P(("dp", "cp"), None, None)
    lse_spec = P(("dp", "cp"), None)

    def local_attention(q_tok, k_tok, v_tok):
        tok_count, q_heads, head_dim = q_tok.shape
        kv_heads = k_tok.shape[1]
        group = q_heads // kv_heads
        half_len = tok_count // 2
        rows = group * half_len
        n_item = n_cp // 2 * kv_heads
        q_in = q_tok.transpose(1, 0, 2).reshape(q_heads, 2, half_len, head_dim)
        k_in = k_tok.reshape(tok_count * kv_heads, head_dim)
        v_in = v_tok.reshape(tok_count * kv_heads, head_dim)
        q_in, k_in, v_in = (pltpu.with_memory_space_constraint(x, pltpu.HBM) for x in (q_in, k_in, v_in))
        vmem = pl.BlockSpec(memory_space=pltpu.VMEM)
        hbm = pl.BlockSpec(memory_space=pltpu.HBM)
        out, lse = pl.pallas_call(
            functools.partial(attention_kernel, n_cp),
            out_shape=(pltpu.VMEM(q_in.shape, BF16), pltpu.VMEM((q_heads, tok_count), F32)),
            in_specs=[hbm, hbm, hbm],
            out_specs=(vmem, vmem),
            scratch_shapes=[
                pltpu.VMEM(q_in.shape, BF16),
                pltpu.VMEM((2, n_cp // 2, kv_heads, 2, 2, half_len, head_dim), BF16),
                pltpu.VMEM((2, tok_count * kv_heads, head_dim), BF16),
                pltpu.VMEM((2, tok_count * kv_heads, head_dim), F32),
                pltpu.VMEM((2, kv_heads, head_dim, rows), F32),
                pltpu.VMEM((2, kv_heads, 1, rows), F32),
                pltpu.VMEM((2, kv_heads, 8, rows), F32),
                pltpu.SemaphoreType.DMA((n_item,)),
                pltpu.SemaphoreType.DMA((n_item,)),
                pltpu.SemaphoreType.DMA((n_item + 2 * kv_heads,)),
                pltpu.SemaphoreType.DMA((n_item + 2 * kv_heads,)),
                pltpu.SemaphoreType.DMA((7,)),
                pltpu.SemaphoreType.REGULAR,
            ],
            compiler_params=pltpu.CompilerParams(
                collective_id=0, has_side_effects=True,
                vmem_limit_bytes=48 * 1024 * 1024),
        )(q_in, k_in, v_in)
        out, lse = pl.pallas_call(
            store_kernel,
            out_shape=(jax.ShapeDtypeStruct(out.shape, BF16), jax.ShapeDtypeStruct(lse.shape, F32)),
            in_specs=[vmem, vmem],
            out_specs=(hbm, hbm),
            scratch_shapes=[pltpu.SemaphoreType.DMA((2,))],
            compiler_params=pltpu.CompilerParams(vmem_limit_bytes=48 * 1024 * 1024),
        )(out, lse)
        out_tok = out.reshape(q_heads, tok_count, head_dim).transpose(1, 0, 2)
        return out_tok, lse.T

    return jax.shard_map(local_attention, mesh=mesh, in_specs=(row_spec, row_spec, row_spec),
                         out_specs=(row_spec, lse_spec), check_vma=False)
```
